32 devices in a mesh: batch: 1 (over z), row: 4 (over y), col: 8 (over x, core).
Axes of the slice: x: 4, y: 4, z: 1, core: 2. Of those that a mesh axis runs over, the one named last changes fastest.
The devices are a block of a 4x4x8 slice.
Arguments:
- a_mat: bfloat16 [7168, 7168], P(('batch', 'row'), 'col')
- x_start: float32 [7168, 256], P(('batch', 'row', 'col'))
- shifts: float32 [32], P('batch')
Outputs:
- output 1: float32 [7168, 256], P(('batch', 'row', 'col'))
- output 2: float32 [256, 256], P('batch')
All inputs are finite; a program needn't handle non-finite values.
Results may differ from the reference program's by a relative error of at most 0.00141845.
Values are sent between devices in bfloat16 or wider.
A program may use at most 768 MiB of HBM per device.

```python
import math
import jax
import jax.numpy as jnp
from jax import lax

MATRIX_DIM = 7168
BLOCK_WIDTH = 256
SWEEPS = 32


def setup_inputs(seed: int = 0, part: int = 0) -> dict:
    base_key = jax.random.fold_in(jax.random.key(seed), part)
    key_vec, key_val, key_noise, key_start, key_shift = jax.random.split(base_key, 5)
    eig_basis, _ = jnp.linalg.qr(jax.random.normal(key_vec, (MATRIX_DIM, BLOCK_WIDTH), jnp.float32))
    top_vals = jnp.exp(jax.random.uniform(key_val, (BLOCK_WIDTH,), jnp.float32, math.log(1.3), math.log(9.3)))
    low_rank = jnp.dot(eig_basis * top_vals, eig_basis.T)
    noise_mat = jax.random.normal(key_noise, (MATRIX_DIM, MATRIX_DIM), jnp.float32)
    noise_scale = 0.15 / math.sqrt(2.0 * MATRIX_DIM)
    dense_op = 0.5 * (low_rank + low_rank.T) + noise_scale * (noise_mat + noise_mat.T)
    dense_op = dense_op + 0.7 * jnp.eye(MATRIX_DIM, dtype=jnp.float32)
    x_start = jax.random.normal(key_start, (MATRIX_DIM, BLOCK_WIDTH), jnp.float32)
    shifts = jax.random.uniform(key_shift, (SWEEPS,), jnp.float32, -0.6, 0.2)
    return {"a_mat": dense_op.astype(jnp.bfloat16), "x_start": x_start, "shifts": shifts}


def orthonormalize(y_blk):
    y_low = y_blk.astype(jnp.bfloat16)
    gram_one = jnp.dot(y_low.T, y_low, preferred_element_type=jnp.float32) / MATRIX_DIM
    chol_one = jnp.linalg.cholesky(gram_one)
    y_mid = lax.linalg.triangular_solve(chol_one, y_blk, left_side=False, lower=True, transpose_a=True)
    gram_two = jnp.dot(y_mid.T, y_mid, precision=lax.Precision.HIGHEST) / MATRIX_DIM
    chol_two = jnp.linalg.cholesky(gram_two)
    return lax.linalg.triangular_solve(chol_two, y_mid, left_side=False, lower=True, transpose_a=True)


def reference(a_mat, x_start, shifts):
    def sweep(x_cur, shift_val):
        applied = jnp.dot(a_mat, x_cur.astype(jnp.bfloat16), preferred_element_type=jnp.float32)
        return orthonormalize(applied - shift_val * x_cur), None

    x_final, _ = lax.scan(sweep, x_start, shifts)
    ax_final = jnp.dot(a_mat, x_final.astype(jnp.bfloat16), preferred_element_type=jnp.float32)
    rayleigh = jnp.dot(x_final.T, ax_final, precision=lax.Precision.HIGHEST) / MATRIX_DIM
    return x_final, rayleigh
```

```python
import functools

import jax
import jax.numpy as jnp
from jax import lax
from jax.experimental import pallas as pl
from jax.experimental.pallas import tpu as pltpu
from jax.sharding import PartitionSpec as P

HI = lax.Precision.HIGHEST
ROW_CONTRACT = (((0,), (0,)), ((), ()))
GRID_AXES = ("row", "col")
NB = 32
FIRST_ERR = 1e-2
SECOND_ERR = 1.6e-7
LINE = (0, 1, -1, 2)
MESH_ID = pl.DeviceIdType.MESH


def factor_panel(panel, start, nb):
    width = panel.shape[1]
    tiles = width // 128
    groups = nb // 8
    p = [[panel[8*v:8*v+8, 128*t:128*t+128] for t in range(tiles)] for v in range(groups)]
    sub = lax.broadcasted_iota(jnp.int32, (8, 128), 0)
    lane = lax.broadcasted_iota(jnp.int32, (8, 128), 1)
    dinv = [None]*groups
    for g in range(groups):
        cols = [start + 8*g + j for j in range(8)]
        b = [[jnp.broadcast_to(p[v][c//128][:, c%128:c%128+1], (8, 128)) for v in range(g, groups)] for c in cols]
        dg = jnp.ones((8, 128), jnp.float32)
        for j in range(8):
            c = cols[j]
            tc = c // 128
            d = jnp.broadcast_to(b[j][0][j:j+1, :], (8, 128))
            inv = 1.0 / d
            dg = jnp.where(sub == j, inv, dg)
            m = [b[j][v]*inv for v in range(groups-g)]
            for q in range(j+1, 8):
                f = jnp.broadcast_to(b[q][0][j:j+1, :], (8, 128))
                b[q] = [b[q][v] - m[v]*f for v in range(groups-g)]
            m[0] = jnp.where(sub > j, m[0], 0.0)
            for t in range(tiles):
                r = jnp.broadcast_to(p[g][t][j:j+1, :], (8, 128))
                if t == tc:
                    r = jnp.where(lane == c % 128, 1.0, r)
                for v in range(g, groups):
                    old = p[v][t]
                    if t == tc:
                        old = jnp.where(lane == c % 128, jnp.where(sub == j, 1.0, 0.0) if v == g else 0.0, old)
                    p[v][t] = old - m[v-g]*r
            for v in range(g):
                p[v][tc] = jnp.where(lane == c % 128, 0.0, p[v][tc])
        dinv[g] = dg
    rows = []
    for v in range(groups):
        s = jnp.sqrt(dinv[v])
        rows.append(jnp.concatenate([p[v][t]*s for t in range(tiles)], axis=1))
    return jnp.concatenate(rows, axis=0)


def chol_inverse(w_ref, nb=NB):
    size = w_ref.shape[0]
    for k in range(size // nb):
        lo, hi = k*nb, (k+1)*nb
        panel = factor_panel(w_ref[lo:hi, :], lo, nb)
        w_ref[lo:hi, :] = panel
        if hi < size:
            upd = lax.dot_general(panel, panel, (((0,), (0,)), ((), ())), precision=HI, preferred_element_type=jnp.float32)
            upd = upd[hi:, :]
            lane = lax.broadcasted_iota(jnp.int32, (size-hi, size), 1)
            old = w_ref[hi:, :]
            old = jnp.where((lane >= lo) & (lane < hi), 0.0, old)
            w_ref[hi:, :] = old - upd


def lower_mask(x):
    r = lax.broadcasted_iota(jnp.int32, x.shape, 0)
    c = lax.broadcasted_iota(jnp.int32, x.shape, 1)
    return jnp.where(r >= c, x, 0.0)


def cholesky_inverse_kernel(g_ref, o_ref, work):
    work[...] = g_ref[...]
    chol_inverse(work)
    o_ref[...] = lower_mask(work[...])


def cholesky_inverse(gram):
    return pl.pallas_call(
        cholesky_inverse_kernel,
        out_shape=jax.ShapeDtypeStruct(gram.shape, jnp.float32),
        in_specs=[pl.BlockSpec(memory_space=pltpu.VMEM)],
        out_specs=pl.BlockSpec(memory_space=pltpu.VMEM),
        scratch_shapes=[pltpu.VMEM(gram.shape, jnp.float32)],
    )(gram)


def apply_inverse(y_loc, factor_inv):
    return lax.dot_general(y_loc, factor_inv, (((1,), (1,)), ((), ())), precision=HI, preferred_element_type=jnp.float32)


def orthonormalize(y_loc, total_rows):
    y_low = y_loc.astype(jnp.bfloat16)
    gram_one = lax.psum(lax.dot_general(y_low, y_low, ROW_CONTRACT, preferred_element_type=jnp.float32), GRID_AXES) / total_rows
    y_mid = apply_inverse(y_loc, cholesky_inverse(gram_one))
    gram_two = lax.psum(lax.dot_general(y_mid, y_mid, ROW_CONTRACT, precision=HI, preferred_element_type=jnp.float32), GRID_AXES) / total_rows
    return apply_inverse(y_mid, cholesky_inverse(gram_two))

def lower_half(err):
    r = lax.broadcasted_iota(jnp.int32, err.shape, 0)
    c = lax.broadcasted_iota(jnp.int32, err.shape, 1)
    return jnp.where(r > c, err, jnp.where(r == c, 0.5 * err, 0.0))


def eye(size):
    return jnp.where(lax.broadcasted_iota(jnp.int32, (size, size), 0) == lax.broadcasted_iota(jnp.int32, (size, size), 1), 1.0, 0.0)


def mul(a, b):
    return jnp.dot(a, b, precision=HI, preferred_element_type=jnp.float32)


def mul_t(a, b):
    return lax.dot_general(a, b, (((1,), (1,)), ((), ())), precision=HI, preferred_element_type=jnp.float32)


def factor_kernel(total_rows, y_ref, g_ref, flag_ref, x_ref, xlow_ref, flag_out, work):
    scale = 1.0 / total_rows
    work[...] = g_ref[0] * scale
    chol_inverse(work)
    first = lower_mask(work[...])
    unit = eye(work.shape[0])
    gram_two = mul_t(mul(first, g_ref[1] * scale), first)
    err = gram_two - unit
    far_one = jnp.where(jnp.sum(err * err) <= FIRST_ERR, 0.0, 1.0)
    second = unit - lower_half(err)
    err = mul_t(mul(second, gram_two), second) - unit
    far_two = jnp.where(jnp.sum(err * err) <= SECOND_ERR, 0.0, 1.0)
    flag_out[...] = jnp.maximum(flag_ref[...], jnp.maximum(far_one, far_two))
    second = second - mul(lower_half(err), second)
    x_val = mul_t(y_ref[...], mul(second, first))
    x_ref[...] = x_val
    xlow_ref[...] = x_val.astype(jnp.bfloat16)


def factor_and_apply(total_rows, y_loc, grams, flag):
    vmem = pl.BlockSpec(memory_space=pltpu.VMEM)
    return pl.pallas_call(
        functools.partial(factor_kernel, total_rows),
        out_shape=(
            jax.ShapeDtypeStruct(y_loc.shape, jnp.float32),
            jax.ShapeDtypeStruct(y_loc.shape, jnp.bfloat16),
            jax.ShapeDtypeStruct(flag.shape, jnp.float32),
        ),
        in_specs=[vmem] * 3,
        out_specs=(vmem,) * 3,
        scratch_shapes=[pltpu.VMEM(grams.shape[1:], jnp.float32)],
        name="factor_and_apply",
    )(y_loc, grams, flag)


def sweep_kernel(dims, final, shift_ref, index_ref, a_hbm, xlow_ref, x_ref, y_ref, g_ref,
                 a_buf, xbuf, acc, gloc, rhalf, ghalf, slots, red, gsum,
                 a_sem, send_near, recv_near, send_far, recv_far, send_line, recv_line, send_end, recv_end,
                 send_core, recv_core, send_half, recv_half, send_rs, recv_rs, send_bc, recv_bc, send_out, recv_out):
    rows_y, cols, rows = dims
    chips_x = cols // 2
    half = rows // 2
    row, col = lax.axis_index("row"), lax.axis_index("col")
    chip, core = lax.div(col, 2), lax.rem(col, 2)
    size = x_ref.shape[1]
    lanes = size // 2
    part = size // 2
    strip = part // (rows_y * chips_x)

    def place(dx, dy):
        return lax.rem(chip + dx + chips_x, chips_x), lax.rem(row + dy + rows_y, rows_y)

    def device(dx, dy, flip=False):
        px, py = place(dx, dy)
        return {"row": py, "col": px * 2 + ((1 - core) if flip else core)}

    def slot(dx, dy):
        px, py = place(dx, dy)
        return py * chips_x + px

    def axis_pair(h, u, v):
        return (u, v) if h == 0 else (v, u)

    plane = [(dx, dy) for dy in LINE for dx in LINE if (dx, dy) != (0, 0)]
    barrier = pltpu.get_barrier_semaphore()
    for dx, dy in plane:
        pl.semaphore_signal(barrier, inc=1, device_id=device(dx, dy), device_id_type=MESH_ID)
    pl.semaphore_signal(barrier, inc=1, device_id=device(0, 0, True), device_id_type=MESH_ID)
    pl.semaphore_wait(barrier, len(plane) + 1)

    load_a = pltpu.make_async_copy(a_hbm, a_buf, a_sem)
    load_a.start()

    sent = []

    def send(src, dst, ssem, rsem, dev):
        copy = pltpu.make_async_remote_copy(src_ref=src, dst_ref=dst, send_sem=ssem, recv_sem=rsem, device_id=dev, device_id_type=MESH_ID)
        copy.start()
        sent.append(copy)
        return copy

    base = pl.multiple_of(core * rows, 32)

    def unit(h, dx, dy, lane=None):
        where = pl.ds(pl.multiple_of(base + h * half, 16), half)
        if lane is None:
            return xbuf.at[slot(dx, dy), where, :]
        return xbuf.at[slot(dx, dy), where, pl.ds(lane * lanes, lanes)]

    def own(h):
        return xlow_ref.at[pl.ds(h * half, half), :]

    near, far, line, end, cross = {}, {}, {}, {}, {}

    def start_near(h, d):
        near[h, d] = send(own(h), unit(h, 0, 0), send_near.at[h, (d + 1) // 2], recv_near.at[h, (d + 1) // 2], device(*axis_pair(h, d, 0)))

    def start_far(h, d):
        piece = unit(h, *axis_pair(h, -d, 0), lane=(d + 1) // 2)
        far[h, d] = send(piece, piece, send_far.at[h, (d + 1) // 2], recv_far.at[h, (d + 1) // 2], device(*axis_pair(h, d, 0)))

    def start_line(h, u):
        for d in (1, -1):
            piece = unit(h, *axis_pair(h, u, 0))
            line[h, u, d] = send(own(h) if u == 0 else piece, piece, send_line.at[h, u + 1, (d + 1) // 2], recv_line.at[h, u + 1, (d + 1) // 2],
                                 device(*axis_pair(h, 0, d)))

    def start_end(h, u, d):
        piece = unit(h, *axis_pair(h, u, -d), lane=(d + 1) // 2)
        end[h, u, d] = send(piece, piece, send_end.at[h, u + 1, (d + 1) // 2], recv_end.at[h, u + 1, (d + 1) // 2], device(*axis_pair(h, 0, d)))

    def start_cross(dx, dy):
        block = xbuf.at[slot(dx, dy), pl.ds(base, rows), :]
        index = (dy + 1) * 4 + dx + 1
        cross[dx, dy] = send(xlow_ref if (dx, dy) == (0, 0) else block, block, send_core.at[index], recv_core.at[index], device(0, 0, True))

    def product(dx, dy, first=False):
        cross[dx, dy].wait_recv()
        term = jnp.dot(a_buf[slot(dx, dy)], xbuf[slot(dx, dy)], preferred_element_type=jnp.float32)
        acc[...] = term if first else acc[...] + term

    for d in (1, -1):
        for h in (0, 1):
            start_near(h, d)
    for h in (0, 1):
        start_line(h, 0)
    start_cross(0, 0)
    xbuf[slot(0, 0), pl.ds(base, rows), :] = xlow_ref[...]
    for d in (1, -1):
        for h in (0, 1):
            near[h, d].wait_recv()
            start_far(h, d)
            start_line(h, -d)
    for d in (1, -1):
        for h in (0, 1):
            line[h, 0, d].wait_recv()
            start_end(h, 0, d)
    for d in (1, -1):
        start_cross(d, 0)
        start_cross(0, d)
    load_a.wait()
    product(0, 0, first=True)
    for h in (0, 1):
        for d in (1, -1):
            far[h, d].wait_recv()
        start_line(h, 2)
    for u in (1, -1):
        for d in (1, -1):
            for h in (0, 1):
                line[h, u, d].wait_recv()
                start_end(h, u, d)
    for u in (1, -1):
        for d in (1, -1):
            start_cross(u, d)
    for d in (1, -1):
        product(d, 0)
        product(0, d)
    for h in (0, 1):
        for d in (1, -1):
            end[h, 0, d].wait_recv()
    start_cross(2, 0)
    start_cross(0, 2)
    for d in (1, -1):
        for h in (0, 1):
            line[h, 2, d].wait_recv()
            start_end(h, 2, d)
    for u in (1, -1):
        for d in (1, -1):
            product(u, d)
    for u in (1, -1):
        for h in (0, 1):
            for d in (1, -1):
                end[h, u, d].wait_recv()
    for u in (1, -1):
        start_cross(2, u)
        start_cross(u, 2)
    product(2, 0)
    product(0, 2)
    for h in (0, 1):
        for d in (1, -1):
            end[h, 2, d].wait_recv()
    start_cross(2, 2)
    for u in (1, -1):
        product(2, u)
        product(u, 2)
    product(2, 2)

    if final:
        y_ref[...] = acc[...]
        gloc[0] = lax.dot_general(x_ref[...], acc[...], ROW_CONTRACT, precision=HI, preferred_element_type=jnp.float32)
    else:
        y_val = acc[...] - shift_ref[index_ref[0]] * x_ref[...]
        y_ref[...] = y_val
        y_low = y_val.astype(jnp.bfloat16)
        gloc[0] = lax.dot_general(y_low, y_low, ROW_CONTRACT, preferred_element_type=jnp.float32)
        gloc[1] = lax.dot_general(y_val, y_val, ROW_CONTRACT, precision=HI, preferred_element_type=jnp.float32)

    kept = pl.ds(pl.multiple_of(core * part, 8), part)
    given = pl.ds(pl.multiple_of((1 - core) * part, 8), part)
    send(gloc.at[:, given, :], rhalf, send_half, recv_half, device(0, 0, True)).wait_recv()
    ghalf[...] = gloc[:, kept, :] + rhalf[...]
    mine = slot(0, 0)
    waits = []
    for n, (dx, dy) in enumerate(plane):
        rows_of = pl.ds(pl.multiple_of(slot(dx, dy) * strip, 8), strip)
        waits.append(send(ghalf.at[:, rows_of, :], slots.at[mine], send_rs.at[n], recv_rs.at[n], device(dx, dy)))
    slots[mine] = ghalf[:, pl.ds(pl.multiple_of(mine * strip, 8), strip), :]
    for copy in waits:
        copy.wait_recv()
    red[...] = jnp.sum(slots[...], axis=0)
    waits = []
    mine_rows = pl.ds(pl.multiple_of(core * part + mine * strip, 8), strip)
    for n, (dx, dy) in enumerate(plane):
        waits.append(send(red, gsum.at[:, mine_rows, :], send_bc.at[n], recv_bc.at[n], device(dx, dy)))
    gsum[:, mine_rows, :] = red[...]
    for copy in waits:
        copy.wait_recv()
    send(gsum.at[:, kept, :], gsum.at[:, kept, :], send_out, recv_out, device(0, 0, True)).wait_recv()
    g_ref[...] = gsum[...]
    for copy in sent:
        copy.wait_send()


def group_product(dims, final, shifts, index, a_blocks, x_low, x_loc):
    rows_y, cols, rows = dims
    size = x_loc.shape[1]
    chips = rows_y * cols // 2
    grams = 1 if final else 2
    dma = pltpu.SemaphoreType.DMA
    vmem = pl.BlockSpec(memory_space=pltpu.VMEM)
    smem = pl.BlockSpec(memory_space=pltpu.SMEM)
    peers = chips - 1
    return pl.pallas_call(
        functools.partial(sweep_kernel, dims, final),
        out_shape=(jax.ShapeDtypeStruct((rows, size), jnp.float32), jax.ShapeDtypeStruct((grams, size, size), jnp.float32)),
        in_specs=[smem, smem, pl.BlockSpec(memory_space=pl.ANY), vmem, vmem],
        out_specs=(vmem, vmem),
        scratch_shapes=[
            pltpu.VMEM(a_blocks.shape, jnp.bfloat16),
            pltpu.VMEM((chips, 2 * rows, size), jnp.bfloat16),
            pltpu.VMEM((rows, size), jnp.float32),
            pltpu.VMEM((grams, size, size), jnp.float32),
            pltpu.VMEM((grams, size // 2, size), jnp.float32),
            pltpu.VMEM((grams, size // 2, size), jnp.float32),
            pltpu.VMEM((chips, grams, size // 2 // chips, size), jnp.float32),
            pltpu.VMEM((grams, size // 2 // chips, size), jnp.float32),
            pltpu.VMEM((grams, size, size), jnp.float32),
            dma,
            dma((2, 2)), dma((2, 2)), dma((2, 2)), dma((2, 2)),
            dma((2, 4, 2)), dma((2, 4, 2)), dma((2, 4, 2)), dma((2, 4, 2)),
            dma((16,)), dma((16,)), dma, dma,
            dma((peers,)), dma((peers,)), dma((peers,)), dma((peers,)), dma, dma,
        ],
        compiler_params=pltpu.CompilerParams(collective_id=1 if final else 0, has_side_effects=True, vmem_limit_bytes=56 * 2**20),
        name="final_product" if final else "sweep_product",
    )(shifts, index, a_blocks, x_low, x_loc)


def solution(mesh):
    row_count = mesh.shape["row"]
    col_count = mesh.shape["col"]

    def apply_operator(a_rows, x_loc):
        x_full = lax.all_gather(x_loc.astype(jnp.bfloat16), GRID_AXES, axis=0, tiled=True)
        return jnp.dot(a_rows, x_full, preferred_element_type=jnp.float32)

    def careful_program(a_rows, x_loc, shift_vec, total_rows):
        def sweep(sweep_idx, x_cur):
            applied = apply_operator(a_rows, x_cur)
            return orthonormalize(applied - shift_vec[sweep_idx] * x_cur, total_rows)

        x_loc = lax.fori_loop(0, shift_vec.shape[0], sweep, x_loc)
        applied = apply_operator(a_rows, x_loc)
        local_part = lax.dot_general(x_loc, applied, ROW_CONTRACT, precision=HI, preferred_element_type=jnp.float32)
        return x_loc, lax.psum(local_part, GRID_AXES) / total_rows

    def local_program(a_blk, x_start, shift_vec):
        total_rows = a_blk.shape[0] * row_count
        rows = x_start.shape[0]
        dims = (row_count, col_count, rows)
        a_rows = lax.all_to_all(a_blk, "col", split_axis=0, concat_axis=1, tiled=True)
        a_blocks = a_rows.reshape(rows, row_count * col_count // 2, 2 * rows).transpose(1, 0, 2)

        def sweep(sweep_idx, carry):
            x_loc, x_low, flag = carry
            y_loc, grams = group_product(dims, False, shift_vec, jnp.full((1,), sweep_idx, jnp.int32), a_blocks, x_low, x_loc)
            return factor_and_apply(total_rows, y_loc, grams, flag)

        start = (x_start, x_start.astype(jnp.bfloat16), jnp.zeros((8, 128), jnp.float32))
        x_loc, x_low, flag = lax.fori_loop(0, shift_vec.shape[0], sweep, start)
        _, total = group_product(dims, True, shift_vec, jnp.zeros((1,), jnp.int32), a_blocks, x_low, x_loc)
        return lax.cond(
            flag[0, 0] > 0.0,
            lambda: careful_program(a_rows, x_start, shift_vec, total_rows),
            lambda: (x_loc, total[0] / total_rows),
        )

    return jax.shard_map(
        local_program,
        mesh=mesh,
        in_specs=(P(("batch", "row"), "col"), P(("batch", "row", "col"), None), P("batch")),
        out_specs=(P(("batch", "row", "col"), None), P("batch", None)),
        check_vma=False,
    )
```

```python
import functools

import jax
import jax.numpy as jnp
from jax import lax
from jax.experimental import pallas as pl
from jax.experimental.pallas import tpu as pltpu
from jax.sharding import PartitionSpec as P

HI = lax.Precision.HIGHEST
ROW_CONTRACT = (((0,), (0,)), ((), ()))
GRID_AXES = ("row", "col")
NB = 32
FIRST_ERR = 1e-2
SECOND_ERR = 1.6e-7
LINE = (0, 1, -1, 2)
MESH_ID = pl.DeviceIdType.MESH


def factor_panel(panel, start, nb):
    width = panel.shape[1]
    tiles = width // 128
    groups = nb // 8
    p = [[panel[8*v:8*v+8, 128*t:128*t+128] for t in range(tiles)] for v in range(groups)]
    sub = lax.broadcasted_iota(jnp.int32, (8, 128), 0)
    lane = lax.broadcasted_iota(jnp.int32, (8, 128), 1)
    dinv = [None]*groups
    for g in range(groups):
        cols = [start + 8*g + j for j in range(8)]
        b = [[jnp.broadcast_to(p[v][c//128][:, c%128:c%128+1], (8, 128)) for v in range(g, groups)] for c in cols]
        dg = jnp.ones((8, 128), jnp.float32)
        for j in range(8):
            c = cols[j]
            tc = c // 128
            d = jnp.broadcast_to(b[j][0][j:j+1, :], (8, 128))
            inv = 1.0 / d
            dg = jnp.where(sub == j, inv, dg)
            m = [b[j][v]*inv for v in range(groups-g)]
            for q in range(j+1, 8):
                f = jnp.broadcast_to(b[q][0][j:j+1, :], (8, 128))
                b[q] = [b[q][v] - m[v]*f for v in range(groups-g)]
            m[0] = jnp.where(sub > j, m[0], 0.0)
            for t in range(tiles):
                r = jnp.broadcast_to(p[g][t][j:j+1, :], (8, 128))
                if t == tc:
                    r = jnp.where(lane == c % 128, 1.0, r)
                for v in range(g, groups):
                    old = p[v][t]
                    if t == tc:
                        old = jnp.where(lane == c % 128, jnp.where(sub == j, 1.0, 0.0) if v == g else 0.0, old)
                    p[v][t] = old - m[v-g]*r
            for v in range(g):
                p[v][tc] = jnp.where(lane == c % 128, 0.0, p[v][tc])
        dinv[g] = dg
    rows = []
    for v in range(groups):
        s = jnp.sqrt(dinv[v])
        rows.append(jnp.concatenate([p[v][t]*s for t in range(tiles)], axis=1))
    return jnp.concatenate(rows, axis=0)


def chol_inverse(w_ref, hooks={}, nb=NB):
    size = w_ref.shape[0]
    for k in range(size // nb):
        lo, hi = k*nb, (k+1)*nb
        panel = factor_panel(w_ref[lo:hi, :], lo, nb)
        w_ref[lo:hi, :] = panel
        if k in hooks:
            hooks[k]()
        if hi < size:
            upd = lax.dot_general(panel, panel, (((0,), (0,)), ((), ())), precision=HI, preferred_element_type=jnp.float32)
            upd = upd[hi:, :]
            lane = lax.broadcasted_iota(jnp.int32, (size-hi, size), 1)
            old = w_ref[hi:, :]
            old = jnp.where((lane >= lo) & (lane < hi), 0.0, old)
            w_ref[hi:, :] = old - upd


def lower_mask(x):
    r = lax.broadcasted_iota(jnp.int32, x.shape, 0)
    c = lax.broadcasted_iota(jnp.int32, x.shape, 1)
    return jnp.where(r >= c, x, 0.0)


def cholesky_inverse_kernel(g_ref, o_ref, work):
    work[...] = g_ref[...]
    chol_inverse(work)
    o_ref[...] = lower_mask(work[...])


def cholesky_inverse(gram):
    return pl.pallas_call(
        cholesky_inverse_kernel,
        out_shape=jax.ShapeDtypeStruct(gram.shape, jnp.float32),
        in_specs=[pl.BlockSpec(memory_space=pltpu.VMEM)],
        out_specs=pl.BlockSpec(memory_space=pltpu.VMEM),
        scratch_shapes=[pltpu.VMEM(gram.shape, jnp.float32)],
    )(gram)


def apply_inverse(y_loc, factor_inv):
    return lax.dot_general(y_loc, factor_inv, (((1,), (1,)), ((), ())), precision=HI, preferred_element_type=jnp.float32)


def orthonormalize(y_loc, total_rows):
    y_low = y_loc.astype(jnp.bfloat16)
    gram_one = lax.psum(lax.dot_general(y_low, y_low, ROW_CONTRACT, preferred_element_type=jnp.float32), GRID_AXES) / total_rows
    y_mid = apply_inverse(y_loc, cholesky_inverse(gram_one))
    gram_two = lax.psum(lax.dot_general(y_mid, y_mid, ROW_CONTRACT, precision=HI, preferred_element_type=jnp.float32), GRID_AXES) / total_rows
    return apply_inverse(y_mid, cholesky_inverse(gram_two))

def lower_half(err):
    r = lax.broadcasted_iota(jnp.int32, err.shape, 0)
    c = lax.broadcasted_iota(jnp.int32, err.shape, 1)
    return jnp.where(r > c, err, jnp.where(r == c, 0.5 * err, 0.0))


def eye(size):
    return jnp.where(lax.broadcasted_iota(jnp.int32, (size, size), 0) == lax.broadcasted_iota(jnp.int32, (size, size), 1), 1.0, 0.0)


def mul(a, b):
    return jnp.dot(a, b, precision=HI, preferred_element_type=jnp.float32)


def mul_t(a, b):
    return lax.dot_general(a, b, (((1,), (1,)), ((), ())), precision=HI, preferred_element_type=jnp.float32)


def subspace_kernel(dims, total_rows, shift_ref, a_hbm, start_ref, x_ref, h_ref, flag_ref,
                    a_buf, xlow, xbuf, acc, gloc, rhalf, ghalf, slots, red, gsum, work,
                    a_sem, send_near, recv_near, send_far, recv_far, send_line, recv_line, send_end, recv_end,
                    send_core, recv_core, send_half, recv_half, send_rs, recv_rs, send_bc, recv_bc, send_out, recv_out):
    rows_y, cols, rows = dims
    chips_x = cols // 2
    half = rows // 2
    row, col = lax.axis_index("row"), lax.axis_index("col")
    chip, core = lax.div(col, 2), lax.rem(col, 2)
    size = x_ref.shape[1]
    lanes = size // 2
    part = size // 2
    strip = part // (rows_y * chips_x)

    def place(dx, dy):
        return lax.rem(chip + dx + chips_x, chips_x), lax.rem(row + dy + rows_y, rows_y)

    def device(dx, dy, flip=False):
        px, py = place(dx, dy)
        return {"row": py, "col": px * 2 + ((1 - core) if flip else core)}

    def slot(dx, dy):
        px, py = place(dx, dy)
        return py * chips_x + px

    def axis_pair(h, u, v):
        return (u, v) if h == 0 else (v, u)

    plane = [(dx, dy) for dy in LINE for dx in LINE if (dx, dy) != (0, 0)]
    barrier = pltpu.get_barrier_semaphore()
    for dx, dy in plane:
        pl.semaphore_signal(barrier, inc=1, device_id=device(dx, dy), device_id_type=MESH_ID)
    pl.semaphore_signal(barrier, inc=1, device_id=device(0, 0, True), device_id_type=MESH_ID)
    pl.semaphore_wait(barrier, len(plane) + 1)

    load = pltpu.make_async_copy(a_hbm, a_buf, a_sem)
    load.start()

    def gather_product():
        sent = []

        def send(src, dst, ssem, rsem, dev):
            copy = pltpu.make_async_remote_copy(src_ref=src, dst_ref=dst, send_sem=ssem, recv_sem=rsem, device_id=dev, device_id_type=MESH_ID)
            copy.start()
            sent.append(copy)
            return copy

        base = pl.multiple_of(core * rows, 32)

        def unit(h, dx, dy, lane=None):
            where = pl.ds(pl.multiple_of(base + h * half, 16), half)
            if lane is None:
                return xbuf.at[slot(dx, dy), where, :]
            return xbuf.at[slot(dx, dy), where, pl.ds(lane * lanes, lanes)]

        def own(h):
            return xlow.at[pl.ds(h * half, half), :]

        near, far, line, end, cross = {}, {}, {}, {}, {}

        def start_near(h, d):
            near[h, d] = send(own(h), unit(h, 0, 0), send_near.at[h, (d + 1) // 2], recv_near.at[h, (d + 1) // 2], device(*axis_pair(h, d, 0)))

        def start_far(h, d):
            piece = unit(h, *axis_pair(h, -d, 0), lane=(d + 1) // 2)
            far[h, d] = send(piece, piece, send_far.at[h, (d + 1) // 2], recv_far.at[h, (d + 1) // 2], device(*axis_pair(h, d, 0)))

        def start_line(h, u):
            for d in (1, -1):
                piece = unit(h, *axis_pair(h, u, 0))
                line[h, u, d] = send(own(h) if u == 0 else piece, piece, send_line.at[h, u + 1, (d + 1) // 2], recv_line.at[h, u + 1, (d + 1) // 2],
                                     device(*axis_pair(h, 0, d)))

        def start_end(h, u, d):
            piece = unit(h, *axis_pair(h, u, -d), lane=(d + 1) // 2)
            end[h, u, d] = send(piece, piece, send_end.at[h, u + 1, (d + 1) // 2], recv_end.at[h, u + 1, (d + 1) // 2], device(*axis_pair(h, 0, d)))

        def start_cross(dx, dy):
            block = xbuf.at[slot(dx, dy), pl.ds(base, rows), :]
            index = (dy + 1) * 4 + dx + 1
            cross[dx, dy] = send(xlow if (dx, dy) == (0, 0) else block, block, send_core.at[index], recv_core.at[index], device(0, 0, True))

        def product(dx, dy, first=False):
            cross[dx, dy].wait_recv()
            term = jnp.dot(a_buf[slot(dx, dy)], xbuf[slot(dx, dy)], preferred_element_type=jnp.float32)
            acc[...] = term if first else acc[...] + term

        for d in (1, -1):
            for h in (0, 1):
                start_near(h, d)
        for h in (0, 1):
            start_line(h, 0)
        start_cross(0, 0)
        xbuf[slot(0, 0), pl.ds(base, rows), :] = xlow[...]
        for d in (1, -1):
            for h in (0, 1):
                near[h, d].wait_recv()
                start_far(h, d)
                start_line(h, -d)
        for d in (1, -1):
            for h in (0, 1):
                line[h, 0, d].wait_recv()
                start_end(h, 0, d)
        for d in (1, -1):
            start_cross(d, 0)
            start_cross(0, d)
        product(0, 0, first=True)
        for h in (0, 1):
            for d in (1, -1):
                far[h, d].wait_recv()
            start_line(h, 2)
        for u in (1, -1):
            for d in (1, -1):
                for h in (0, 1):
                    line[h, u, d].wait_recv()
                    start_end(h, u, d)
        for u in (1, -1):
            for d in (1, -1):
                start_cross(u, d)
        for d in (1, -1):
            product(d, 0)
            product(0, d)
        for h in (0, 1):
            for d in (1, -1):
                end[h, 0, d].wait_recv()
        start_cross(2, 0)
        start_cross(0, 2)
        for d in (1, -1):
            for h in (0, 1):
                line[h, 2, d].wait_recv()
                start_end(h, 2, d)
        for u in (1, -1):
            for d in (1, -1):
                product(u, d)
        for u in (1, -1):
            for h in (0, 1):
                for d in (1, -1):
                    end[h, u, d].wait_recv()
        for u in (1, -1):
            start_cross(2, u)
            start_cross(u, 2)
        product(2, 0)
        product(0, 2)
        for h in (0, 1):
            for d in (1, -1):
                end[h, 2, d].wait_recv()
        start_cross(2, 2)
        for u in (1, -1):
            product(2, u)
            product(u, 2)
        product(2, 2)

        for copy in sent:
            copy.wait_send()

    kept = pl.ds(pl.multiple_of(core * part, 8), part)
    given = pl.ds(pl.multiple_of((1 - core) * part, 8), part)
    mine = slot(0, 0)
    mine_rows = pl.ds(pl.multiple_of(core * part + mine * strip, 8), strip)

    def send(src, dst, ssem, rsem, dev):
        copy = pltpu.make_async_remote_copy(src_ref=src, dst_ref=dst, send_sem=ssem, recv_sem=rsem, device_id=dev, device_id_type=MESH_ID)
        copy.start()
        return copy

    class GroupSum:
        def __init__(self, n):
            self.n = n
            self.sent = []
            self.waits = [send(gloc.at[n, given, :], rhalf.at[n], send_half.at[n], recv_half.at[n], device(0, 0, True))]

        def arrive(self):
            for copy in self.waits:
                copy.wait_recv()
            self.sent += self.waits
            self.waits = []

        def scatter(self):
            n = self.n
            self.arrive()
            ghalf[n] = gloc[n, kept, :] + rhalf[n]
            for i, (dx, dy) in enumerate(plane):
                rows_of = pl.ds(pl.multiple_of(slot(dx, dy) * strip, 8), strip)
                self.waits.append(send(ghalf.at[n, rows_of, :], slots.at[n, mine], send_rs.at[n, i], recv_rs.at[n, i], device(dx, dy)))
            slots[n, mine] = ghalf[n, pl.ds(pl.multiple_of(mine * strip, 8), strip), :]

        def spread(self):
            n = self.n
            self.arrive()
            red[n] = jnp.sum(slots[n], axis=0)
            for i, (dx, dy) in enumerate(plane):
                self.waits.append(send(red.at[n], gsum.at[n, mine_rows, :], send_bc.at[n, i], recv_bc.at[n, i], device(dx, dy)))
            gsum[n, mine_rows, :] = red[n]

        def cross(self):
            n = self.n
            self.arrive()
            self.waits.append(send(gsum.at[n, kept, :], gsum.at[n, kept, :], send_out.at[n], recv_out.at[n], device(0, 0, True)))

        def finish(self):
            for copy in self.sent:
                copy.wait_send()

    scale = 1.0 / total_rows
    unit_mat = eye(size)

    def sweep(t):
        gather_product()
        y_val = acc[...] - shift_ref[t] * x_ref[...]
        y_low = y_val.astype(jnp.bfloat16)
        gloc[0] = lax.dot_general(y_low, y_low, ROW_CONTRACT, preferred_element_type=jnp.float32)
        one = GroupSum(0)
        acc[...] = y_val
        gloc[1] = lax.dot_general(y_val, y_val, ROW_CONTRACT, precision=HI, preferred_element_type=jnp.float32)
        two = GroupSum(1)
        one.scatter()
        two.scatter()
        one.spread()
        two.spread()
        one.cross()
        one.arrive()
        work[...] = gsum[0] * scale
        chol_inverse(work, {1: two.cross})
        two.arrive()
        first = lower_mask(work[...])
        gram_two = mul_t(mul(first, gsum[1] * scale), first)
        err = gram_two - unit_mat
        far_one = jnp.where(jnp.sum(err * err, axis=(0, 1), keepdims=True) <= FIRST_ERR, 0.0, 1.0)
        second = unit_mat - lower_half(err)
        err = mul_t(mul(second, gram_two), second) - unit_mat
        far_two = jnp.where(jnp.sum(err * err, axis=(0, 1), keepdims=True) <= SECOND_ERR, 0.0, 1.0)
        flag_ref[...] = jnp.maximum(flag_ref[...], jnp.maximum(far_one, far_two))
        second = second - mul(lower_half(err), second)
        x_val = mul_t(acc[...], mul(second, first))
        xlow[...] = x_val.astype(jnp.bfloat16)
        x_ref[...] = x_val
        one.finish()
        two.finish()

    flag_ref[...] = jnp.zeros_like(flag_ref)
    x_ref[...] = start_ref[...]
    xlow[...] = start_ref[...].astype(jnp.bfloat16)
    load.wait()

    @pl.loop(0, shift_ref.shape[0])
    def _(t):
        sweep(t)

    gather_product()
    gloc[0] = lax.dot_general(x_ref[...], acc[...], ROW_CONTRACT, precision=HI, preferred_element_type=jnp.float32)
    total = GroupSum(0)
    total.scatter()
    total.spread()
    total.cross()
    total.arrive()
    h_ref[...] = gsum[0] / total_rows
    total.finish()


def iterate(dims, total_rows, shifts, a_blocks, x_start):
    rows_y, cols, rows = dims
    size = x_start.shape[1]
    chips = rows_y * cols // 2
    dma = pltpu.SemaphoreType.DMA
    vmem = pl.BlockSpec(memory_space=pltpu.VMEM)
    peers = chips - 1
    strip = size // 2 // chips
    return pl.pallas_call(
        functools.partial(subspace_kernel, dims, total_rows),
        out_shape=(
            jax.ShapeDtypeStruct((rows, size), jnp.float32),
            jax.ShapeDtypeStruct((size, size), jnp.float32),
            jax.ShapeDtypeStruct((8, 128), jnp.float32),
        ),
        in_specs=[pl.BlockSpec(memory_space=pltpu.SMEM), pl.BlockSpec(memory_space=pl.ANY), vmem],
        out_specs=(vmem,) * 3,
        scratch_shapes=[
            pltpu.VMEM(a_blocks.shape, jnp.bfloat16),
            pltpu.VMEM((rows, size), jnp.bfloat16),
            pltpu.VMEM((chips, 2 * rows, size), jnp.bfloat16),
            pltpu.VMEM((rows, size), jnp.float32),
            pltpu.VMEM((2, size, size), jnp.float32),
            pltpu.VMEM((2, size // 2, size), jnp.float32),
            pltpu.VMEM((2, size // 2, size), jnp.float32),
            pltpu.VMEM((2, chips, strip, size), jnp.float32),
            pltpu.VMEM((2, strip, size), jnp.float32),
            pltpu.VMEM((2, size, size), jnp.float32),
            pltpu.VMEM((size, size), jnp.float32),
            dma,
            dma((2, 2)), dma((2, 2)), dma((2, 2)), dma((2, 2)),
            dma((2, 4, 2)), dma((2, 4, 2)), dma((2, 4, 2)), dma((2, 4, 2)),
            dma((16,)), dma((16,)), dma((2,)), dma((2,)),
            dma((2, peers)), dma((2, peers)), dma((2, peers)), dma((2, peers)), dma((2,)), dma((2,)),
        ],
        compiler_params=pltpu.CompilerParams(collective_id=0, has_side_effects=True, vmem_limit_bytes=56 * 2**20),
        name="subspace_sweeps",
    )(shifts, a_blocks, x_start)


def solution(mesh):
    row_count = mesh.shape["row"]
    col_count = mesh.shape["col"]

    def apply_operator(a_rows, x_loc):
        x_full = lax.all_gather(x_loc.astype(jnp.bfloat16), GRID_AXES, axis=0, tiled=True)
        return jnp.dot(a_rows, x_full, preferred_element_type=jnp.float32)

    def careful_program(a_rows, x_loc, shift_vec, total_rows):
        def sweep(sweep_idx, x_cur):
            applied = apply_operator(a_rows, x_cur)
            return orthonormalize(applied - shift_vec[sweep_idx] * x_cur, total_rows)

        x_loc = lax.fori_loop(0, shift_vec.shape[0], sweep, x_loc)
        applied = apply_operator(a_rows, x_loc)
        local_part = lax.dot_general(x_loc, applied, ROW_CONTRACT, precision=HI, preferred_element_type=jnp.float32)
        return x_loc, lax.psum(local_part, GRID_AXES) / total_rows

    def local_program(a_blk, x_start, shift_vec):
        total_rows = a_blk.shape[0] * row_count
        rows = x_start.shape[0]
        dims = (row_count, col_count, rows)
        a_rows = lax.all_to_all(a_blk, "col", split_axis=0, concat_axis=1, tiled=True)
        a_blocks = a_rows.reshape(rows, row_count * col_count // 2, 2 * rows).transpose(1, 0, 2)

        x_loc, rayleigh, flag = iterate(dims, total_rows, shift_vec, a_blocks, x_start)
        return lax.cond(
            flag[0, 0] > 0.0,
            lambda: careful_program(a_rows, x_start, shift_vec, total_rows),
            lambda: (x_loc, rayleigh),
        )

    return jax.shard_map(
        local_program,
        mesh=mesh,
        in_specs=(P(("batch", "row"), "col"), P(("batch", "row", "col"), None), P("batch")),
        out_specs=(P(("batch", "row", "col"), None), P("batch", None)),
        check_vma=False,
    )
```

```python
import functools

import jax
import jax.numpy as jnp
from jax import lax
from jax.experimental import pallas as pl
from jax.experimental.pallas import tpu as pltpu
from jax.sharding import PartitionSpec as P

HI = lax.Precision.HIGHEST
ROW_CONTRACT = (((0,), (0,)), ((), ()))
GRID_AXES = ("row", "col")
NB = 32
GRP = 16
FIRST_ERR = 1e-2
SECOND_ERR = 1.6e-7
LINE = (0, 1, -1, 2)
STRAIGHT = (0, 2)
MESH_ID = pl.DeviceIdType.MESH


def factor_panel(panel, other, offset):
    nb = panel.shape[0]
    parts = nb // 8
    p = [panel[8*v:8*v+8, :] for v in range(parts)]
    o = [other[8*v:8*v+8, :] for v in range(parts)]
    sub = lax.broadcasted_iota(jnp.int32, (8, 128), 0)
    lane = lax.broadcasted_iota(jnp.int32, (8, 128), 1)
    scales = [jnp.ones((8, 128), jnp.float32)] * parts
    for first in range(0, nb, GRP):
        b = [{v: jnp.broadcast_to(p[v][:, offset+first+q:offset+first+q+1], (8, 128)) for v in range((first+q)//8, parts)} for q in range(GRP)]
        for q in range(GRP):
            g, j, c = (first + q) // 8, (first + q) % 8, offset + first + q
            inv = 1.0 / jnp.broadcast_to(b[q][g][j:j+1, :], (8, 128))
            scales[g] = jnp.where(sub == j, inv, scales[g])
            m = {v: b[q][v] * inv for v in range(g, parts)}
            for z in range(q+1, GRP):
                gz, jz = (first + z) // 8, (first + z) % 8
                f = jnp.broadcast_to(b[q][gz][jz:jz+1, :], (8, 128))
                for v in range(gz, parts):
                    b[z][v] = b[z][v] - m[v] * f
            m[g] = jnp.where(sub > j, m[g], 0.0)
            row = jnp.where(lane == c, 1.0, jnp.broadcast_to(p[g][j:j+1, :], (8, 128)))
            row_o = jnp.broadcast_to(o[g][j:j+1, :], (8, 128))
            for v in range(parts):
                old = jnp.where(lane == c, jnp.where(sub == j, 1.0, 0.0) if v == g else 0.0, p[v])
                p[v] = old - m[v] * row if v >= g else old
                if v >= g:
                    o[v] = o[v] - m[v] * row_o
    scales = [jnp.sqrt(s) for s in scales]
    return (jnp.concatenate([p[v] * scales[v] for v in range(parts)], axis=0),
            jnp.concatenate([o[v] * scales[v] for v in range(parts)], axis=0))


def chol_inverse(w_ref):
    size = w_ref.shape[0]
    half = size // 2

    @pl.loop(0, 2)
    def _(t):
        here = pl.ds(pl.multiple_of(t * half, half), half)
        there = pl.ds(pl.multiple_of((1 - t) * half, half), half)
        lane = lax.broadcasted_iota(jnp.int32, (NB, half), 1)
        for lo in range(0, half, NB):
            rows = pl.ds(pl.multiple_of(t * half + lo, NB), NB)
            p, o = w_ref[rows, here], w_ref[rows, there]
            p, o = factor_panel(p, o, lo)
            w_ref[rows, here] = p
            w_ref[rows, there] = o
            if lo + NB < half:
                rest = pl.ds(pl.multiple_of(t * half + lo + NB, NB), half - lo - NB)
                lanes = lax.broadcasted_iota(jnp.int32, (half - lo - NB, half), 1)
                u = p[:, lo + NB:]
                old = jnp.where((lanes >= lo) & (lanes < lo + NB), 0.0, w_ref[rest, here])
                w_ref[rest, here] = old - lax.dot_general(u, p, ROW_CONTRACT, precision=HI, preferred_element_type=jnp.float32)
                w_ref[rest, there] = w_ref[rest, there] - lax.dot_general(u, o, ROW_CONTRACT, precision=HI, preferred_element_type=jnp.float32)

        @pl.when(t == 0)
        def _():
            u = w_ref[:half, half:]
            w_ref[half:, half:] = w_ref[half:, half:] - lax.dot_general(u, u, ROW_CONTRACT, precision=HI, preferred_element_type=jnp.float32)
            done = lower_mask(w_ref[:half, :half])
            w_ref[half:, :half] = -lax.dot_general(u, done, ROW_CONTRACT, precision=HI, preferred_element_type=jnp.float32)


def lower_mask(x):
    r = lax.broadcasted_iota(jnp.int32, x.shape, 0)
    c = lax.broadcasted_iota(jnp.int32, x.shape, 1)
    return jnp.where(r >= c, x, 0.0)


def cholesky_inverse_kernel(g_ref, o_ref, work):
    work[...] = g_ref[...]
    chol_inverse(work)
    o_ref[...] = lower_mask(work[...])


def cholesky_inverse(gram):
    return pl.pallas_call(
        cholesky_inverse_kernel,
        out_shape=jax.ShapeDtypeStruct(gram.shape, jnp.float32),
        in_specs=[pl.BlockSpec(memory_space=pltpu.VMEM)],
        out_specs=pl.BlockSpec(memory_space=pltpu.VMEM),
        scratch_shapes=[pltpu.VMEM(gram.shape, jnp.float32)],
    )(gram)


def apply_inverse(y_loc, factor_inv):
    return lax.dot_general(y_loc, factor_inv, (((1,), (1,)), ((), ())), precision=HI, preferred_element_type=jnp.float32)


def orthonormalize(y_loc, total_rows):
    y_low = y_loc.astype(jnp.bfloat16)
    gram_one = lax.psum(lax.dot_general(y_low, y_low, ROW_CONTRACT, preferred_element_type=jnp.float32), GRID_AXES) / total_rows
    y_mid = apply_inverse(y_loc, cholesky_inverse(gram_one))
    gram_two = lax.psum(lax.dot_general(y_mid, y_mid, ROW_CONTRACT, precision=HI, preferred_element_type=jnp.float32), GRID_AXES) / total_rows
    return apply_inverse(y_mid, cholesky_inverse(gram_two))

def lower_half(err):
    r = lax.broadcasted_iota(jnp.int32, err.shape, 0)
    c = lax.broadcasted_iota(jnp.int32, err.shape, 1)
    return jnp.where(r > c, err, jnp.where(r == c, 0.5 * err, 0.0))


def eye(size):
    return jnp.where(lax.broadcasted_iota(jnp.int32, (size, size), 0) == lax.broadcasted_iota(jnp.int32, (size, size), 1), 1.0, 0.0)


def mul(a, b):
    return jnp.dot(a, b, precision=HI, preferred_element_type=jnp.float32)


def mul_t(a, b):
    return lax.dot_general(a, b, (((1,), (1,)), ((), ())), precision=HI, preferred_element_type=jnp.float32)


def subspace_kernel(dims, total_rows, shift_ref, a_hbm, start_ref, x_ref, h_ref, flag_ref,
                    a_buf, xlow, xbuf, acc, gloc, slots, red, gsum, work,
                    a_sem, send_near, recv_near, send_far, recv_far, send_line, recv_line, send_end, recv_end,
                    send_core, recv_core, send_rs, recv_rs, send_bc, recv_bc):
    rows_y, cols, rows = dims
    chips_x = cols // 2
    half = rows // 2
    row, col = lax.axis_index("row"), lax.axis_index("col")
    chip, core = lax.div(col, 2), lax.rem(col, 2)
    size = x_ref.shape[1]
    lanes = size // 2
    strip = size // (rows_y * cols)

    def place(dx, dy):
        return lax.rem(chip + dx + chips_x, chips_x), lax.rem(row + dy + rows_y, rows_y)

    def device(dx, dy, flip=False):
        px, py = place(dx, dy)
        return {"row": py, "col": px * 2 + ((1 - core) if flip else core)}

    def slot(dx, dy):
        px, py = place(dx, dy)
        return py * chips_x + px

    def axis_pair(h, u, v):
        return (u, v) if h == 0 else (v, u)

    peers = [(dx, dy, flip) for dx in LINE for dy in LINE for flip in (False, True) if (dx, dy, flip) != (0, 0, False)]
    peers.sort(key=lambda peer: -(2 * abs(peer[0]) + 2 * abs(peer[1]) + peer[2]))
    barrier = pltpu.get_barrier_semaphore()
    for peer in peers:
        pl.semaphore_signal(barrier, inc=1, device_id=device(*peer), device_id_type=MESH_ID)
    pl.semaphore_wait(barrier, len(peers))

    load = pltpu.make_async_copy(a_hbm, a_buf, a_sem)
    load.start()

    def gather_product():
        sent = []

        def send(src, dst, ssem, rsem, dev):
            copy = pltpu.make_async_remote_copy(src_ref=src, dst_ref=dst, send_sem=ssem, recv_sem=rsem, device_id=dev, device_id_type=MESH_ID)
            copy.start()
            sent.append(copy)
            return copy

        base = pl.multiple_of(core * rows, 32)

        def unit(h, dx, dy, lane=None):
            where = pl.ds(pl.multiple_of(base + h * half, 16), half)
            if lane is None:
                return xbuf.at[slot(dx, dy), where, :]
            return xbuf.at[slot(dx, dy), where, pl.ds(lane * lanes, lanes)]

        def own(h):
            return xlow.at[pl.ds(h * half, half), :]

        near, far, line, end, cross = {}, {}, {}, {}, {}
        signs = (1, -1)

        def start_near(h, d):
            near[h, d] = send(own(h), unit(h, 0, 0), send_near.at[h, (d + 1) // 2], recv_near.at[h, (d + 1) // 2], device(*axis_pair(h, d, 0)))

        def start_far(h):
            far[h] = send(own(h), unit(h, 0, 0), send_far.at[h], recv_far.at[h], device(*axis_pair(h, 2, 0)))

        def start_line(h, u):
            piece = unit(h, *axis_pair(h, u, 0))
            source = own(h) if u == 0 else piece
            for d in signs:
                line[h, u, d] = send(source, piece, send_line.at[h, u + 1, (d + 1) // 2], recv_line.at[h, u + 1, (d + 1) // 2],
                                     device(*axis_pair(h, 0, d)))
            if u in STRAIGHT:
                end[h, u, 1] = send(source, piece, send_end.at[h, u + 1, 0], recv_end.at[h, u + 1, 0], device(*axis_pair(h, 0, 2)))

        def start_end(h, u, d):
            piece = unit(h, *axis_pair(h, u, -d), lane=(d + 1) // 2)
            end[h, u, d] = send(piece, piece, send_end.at[h, u + 1, (d + 1) // 2], recv_end.at[h, u + 1, (d + 1) // 2], device(*axis_pair(h, 0, d)))

        def start_cross(h, dx, dy):
            piece = unit(h, dx, dy)
            index = (dy + 1) * 4 + dx + 1
            cross[h, dx, dy] = send(own(h) if (dx, dy) == (0, 0) else piece, piece, send_core.at[h, index], recv_core.at[h, index], device(0, 0, True))

        def product(dx, dy, first=False):
            for h in (0, 1):
                cross[h, dx, dy].wait_recv()
            term = jnp.dot(a_buf[slot(dx, dy)], xbuf[slot(dx, dy)], preferred_element_type=jnp.float32)
            acc[...] = term if first else acc[...] + term

        def got_line(us):
            for u in us:
                for d in signs:
                    for h in (0, 1):
                        line[h, u, d].wait_recv()
                        if u not in STRAIGHT:
                            start_end(h, u, d)
                        start_cross(h, *axis_pair(h, u, -d))

        def got_end(us):
            for u in us:
                for h in (0, 1):
                    for d in signs:
                        if (h, u, d) in end:
                            end[h, u, d].wait_recv()
                    start_cross(h, *axis_pair(h, u, 2))

        def got_far():
            for h in (0, 1):
                far[h].wait_recv()
                start_line(h, 2)
                start_cross(h, *axis_pair(h, 2, 0))

        for d in signs:
            for h in (0, 1):
                start_near(h, d)
        for h in (0, 1):
            start_far(h)
        for h in (0, 1):
            start_line(h, 0)
            start_cross(h, 0, 0)
        xbuf[slot(0, 0), pl.ds(base, rows), :] = xlow[...]
        for d in signs:
            for h in (0, 1):
                near[h, d].wait_recv()
                start_line(h, -d)
                start_cross(h, *axis_pair(h, -d, 0))
        got_far()
        got_line((0,))
        product(0, 0, first=True)
        got_line((1, -1))
        for d in signs:
            product(d, 0)
            product(0, d)
        got_end((0,))
        got_line((2,))
        product(2, 0)
        product(0, 2)
        for u in signs:
            for d in signs:
                product(u, d)
        got_end((1, -1))
        got_end((2,))
        for u in signs:
            product(2, u)
            product(u, 2)
        product(2, 2)

        for copy in sent:
            copy.wait_send()

    def strip_of(dx, dy, flip):
        px, py = place(dx, dy)
        return py * cols + px * 2 + ((1 - core) if flip else core)

    def strip_rows(index):
        return pl.ds(pl.multiple_of(index * strip, 8), strip)

    mine = strip_of(0, 0, False)

    def send(src, dst, ssem, rsem, dev):
        copy = pltpu.make_async_remote_copy(src_ref=src, dst_ref=dst, send_sem=ssem, recv_sem=rsem, device_id=dev, device_id_type=MESH_ID)
        copy.start()
        return copy

    class GroupSum:
        def __init__(self, n):
            self.n = n
            self.sent = []
            self.waits = [send(gloc.at[n, strip_rows(strip_of(*peer)), :], slots.at[n, mine], send_rs.at[n, i], recv_rs.at[n, i], device(*peer))
                          for i, peer in enumerate(peers)]
            slots[n, mine] = gloc[n, strip_rows(mine), :]

        def arrive(self):
            for copy in self.waits:
                copy.wait_recv()
            self.sent += self.waits
            self.waits = []

        def spread(self):
            n = self.n
            self.arrive()
            red[n] = jnp.sum(slots[n], axis=0)
            self.waits = [send(red.at[n], gsum.at[n, strip_rows(mine), :], send_bc.at[n, i], recv_bc.at[n, i], device(*peer))
                          for i, peer in enumerate(peers)]
            gsum[n, strip_rows(mine), :] = red[n]

        def finish(self):
            for copy in self.sent:
                copy.wait_send()

    scale = 1.0 / total_rows
    unit_mat = eye(size)

    def sweep(t):
        gather_product()
        y_val = acc[...] - shift_ref[t] * x_ref[...]
        y_low = y_val.astype(jnp.bfloat16)
        gloc[0] = lax.dot_general(y_low, y_low, ROW_CONTRACT, preferred_element_type=jnp.float32)
        one = GroupSum(0)
        acc[...] = y_val
        gloc[1] = lax.dot_general(y_val, y_val, ROW_CONTRACT, precision=HI, preferred_element_type=jnp.float32)
        two = GroupSum(1)
        one.spread()
        two.spread()
        one.arrive()
        work[...] = gsum[0] * scale
        chol_inverse(work)
        two.arrive()
        first = lower_mask(work[...])
        gram_two = mul_t(mul(first, gsum[1] * scale), first)
        err = gram_two - unit_mat
        far_one = jnp.where(jnp.sum(err * err, axis=(0, 1), keepdims=True) <= FIRST_ERR, 0.0, 1.0)
        second = unit_mat - lower_half(err)
        near_x = mul_t(acc[...], mul(second, first))
        err = mul_t(mul(second, gram_two), second) - unit_mat
        far_two = jnp.where(jnp.sum(err * err, axis=(0, 1), keepdims=True) <= SECOND_ERR, 0.0, 1.0)
        flag_ref[...] = jnp.maximum(flag_ref[...], jnp.maximum(far_one, far_two))
        x_val = near_x - mul_t(near_x, lower_half(err))
        xlow[...] = x_val.astype(jnp.bfloat16)
        x_ref[...] = x_val
        one.finish()
        two.finish()

    flag_ref[...] = jnp.zeros_like(flag_ref)
    x_ref[...] = start_ref[...]
    xlow[...] = start_ref[...].astype(jnp.bfloat16)
    load.wait()

    @pl.loop(0, shift_ref.shape[0])
    def _(t):
        sweep(t)

    gather_product()
    gloc[0] = lax.dot_general(x_ref[...], acc[...], ROW_CONTRACT, precision=HI, preferred_element_type=jnp.float32)
    total = GroupSum(0)
    total.spread()
    total.arrive()
    h_ref[...] = gsum[0] / total_rows
    total.finish()


def iterate(dims, total_rows, shifts, a_blocks, x_start):
    rows_y, cols, rows = dims
    size = x_start.shape[1]
    chips = rows_y * cols // 2
    dma = pltpu.SemaphoreType.DMA
    vmem = pl.BlockSpec(memory_space=pltpu.VMEM)
    peers = 2 * chips - 1
    strip = size // (2 * chips)
    return pl.pallas_call(
        functools.partial(subspace_kernel, dims, total_rows),
        out_shape=(
            jax.ShapeDtypeStruct((rows, size), jnp.float32),
            jax.ShapeDtypeStruct((size, size), jnp.float32),
            jax.ShapeDtypeStruct((8, 128), jnp.float32),
        ),
        in_specs=[pl.BlockSpec(memory_space=pltpu.SMEM), pl.BlockSpec(memory_space=pl.ANY), vmem],
        out_specs=(vmem,) * 3,
        scratch_shapes=[
            pltpu.VMEM(a_blocks.shape, jnp.bfloat16),
            pltpu.VMEM((rows, size), jnp.bfloat16),
            pltpu.VMEM((chips, 2 * rows, size), jnp.bfloat16),
            pltpu.VMEM((rows, size), jnp.float32),
            pltpu.VMEM((2, size, size), jnp.float32),
            pltpu.VMEM((2, 2 * chips, strip, size), jnp.float32),
            pltpu.VMEM((2, strip, size), jnp.float32),
            pltpu.VMEM((2, size, size), jnp.float32),
            pltpu.VMEM((size, size), jnp.float32),
            dma,
            dma((2, 2)), dma((2, 2)), dma((2,)), dma((2,)),
            dma((2, 4, 2)), dma((2, 4, 2)), dma((2, 4, 2)), dma((2, 4, 2)),
            dma((2, 16)), dma((2, 16)),
            dma((2, peers)), dma((2, peers)), dma((2, peers)), dma((2, peers)),
        ],
        compiler_params=pltpu.CompilerParams(collective_id=0, has_side_effects=True, vmem_limit_bytes=56 * 2**20),
        name="subspace_sweeps",
    )(shifts, a_blocks, x_start)


def solution(mesh):
    row_count = mesh.shape["row"]
    col_count = mesh.shape["col"]

    def apply_operator(a_rows, x_loc):
        x_full = lax.all_gather(x_loc.astype(jnp.bfloat16), GRID_AXES, axis=0, tiled=True)
        return jnp.dot(a_rows, x_full, preferred_element_type=jnp.float32)

    def careful_program(a_rows, x_loc, shift_vec, total_rows):
        def sweep(sweep_idx, x_cur):
            applied = apply_operator(a_rows, x_cur)
            return orthonormalize(applied - shift_vec[sweep_idx] * x_cur, total_rows)

        x_loc = lax.fori_loop(0, shift_vec.shape[0], sweep, x_loc)
        applied = apply_operator(a_rows, x_loc)
        local_part = lax.dot_general(x_loc, applied, ROW_CONTRACT, precision=HI, preferred_element_type=jnp.float32)
        return x_loc, lax.psum(local_part, GRID_AXES) / total_rows

    def local_program(a_blk, x_start, shift_vec):
        total_rows = a_blk.shape[0] * row_count
        rows = x_start.shape[0]
        dims = (row_count, col_count, rows)
        a_rows = lax.all_to_all(a_blk, "col", split_axis=0, concat_axis=1, tiled=True)
        a_blocks = a_rows.reshape(rows, row_count * col_count // 2, 2 * rows).transpose(1, 0, 2)

        x_loc, rayleigh, flag = iterate(dims, total_rows, shift_vec, a_blocks, x_start)
        return lax.cond(
            flag[0, 0] > 0.0,
            lambda: careful_program(a_rows, x_start, shift_vec, total_rows),
            lambda: (x_loc, rayleigh),
        )

    return jax.shard_map(
        local_program,
        mesh=mesh,
        in_specs=(P(("batch", "row"), "col"), P(("batch", "row", "col"), None), P("batch")),
        out_specs=(P(("batch", "row", "col"), None), P("batch", None)),
        check_vma=False,
    )
```

```python
import functools

import jax
import jax.numpy as jnp
from jax import lax
from jax.experimental import pallas as pl
from jax.experimental.pallas import tpu as pltpu
from jax.sharding import PartitionSpec as P

HI = lax.Precision.HIGHEST
ROW_CONTRACT = (((0,), (0,)), ((), ()))
GRID_AXES = ("row", "col")
NB = 32
GRP = 16
FIRST_ERR = 1e-2
SECOND_ERR = 1.6e-7
LINE = (0, 1, -1, 2)
STRAIGHT = (0, 2)
MESH_ID = pl.DeviceIdType.MESH


def factor_panel(panel, other, offset):
    nb = panel.shape[0]
    parts = nb // 8
    p = [panel[8*v:8*v+8, :] for v in range(parts)]
    o = [other[8*v:8*v+8, :] for v in range(parts)]
    sub = lax.broadcasted_iota(jnp.int32, (8, 128), 0)
    lane = lax.broadcasted_iota(jnp.int32, (8, 128), 1)
    scales = [jnp.ones((8, 128), jnp.float32)] * parts
    for first in range(0, nb, GRP):
        b = [{v: jnp.broadcast_to(p[v][:, offset+first+q:offset+first+q+1], (8, 128)) for v in range((first+q)//8, parts)} for q in range(GRP)]
        for q in range(GRP):
            g, j, c = (first + q) // 8, (first + q) % 8, offset + first + q
            inv = 1.0 / jnp.broadcast_to(b[q][g][j:j+1, :], (8, 128))
            scales[g] = jnp.where(sub == j, inv, scales[g])
            m = {v: b[q][v] * inv for v in range(g, parts)}
            for z in range(q+1, GRP):
                gz, jz = (first + z) // 8, (first + z) % 8
                f = jnp.broadcast_to(b[q][gz][jz:jz+1, :], (8, 128))
                for v in range(gz, parts):
                    b[z][v] = b[z][v] - m[v] * f
            m[g] = jnp.where(sub > j, m[g], 0.0)
            row = jnp.where(lane == c, 1.0, jnp.broadcast_to(p[g][j:j+1, :], (8, 128)))
            row_o = jnp.broadcast_to(o[g][j:j+1, :], (8, 128))
            for v in range(parts):
                old = jnp.where(lane == c, jnp.where(sub == j, 1.0, 0.0) if v == g else 0.0, p[v])
                p[v] = old - m[v] * row if v >= g else old
                if v >= g:
                    o[v] = o[v] - m[v] * row_o
    scales = [jnp.sqrt(s) for s in scales]
    return (jnp.concatenate([p[v] * scales[v] for v in range(parts)], axis=0),
            jnp.concatenate([o[v] * scales[v] for v in range(parts)], axis=0))


def chol_inverse(w_ref):
    size = w_ref.shape[0]
    half = size // 2

    @pl.loop(0, 2)
    def _(t):
        here = pl.ds(pl.multiple_of(t * half, half), half)
        there = pl.ds(pl.multiple_of((1 - t) * half, half), half)
        lane = lax.broadcasted_iota(jnp.int32, (NB, half), 1)
        for lo in range(0, half, NB):
            rows = pl.ds(pl.multiple_of(t * half + lo, NB), NB)
            p, o = w_ref[rows, here], w_ref[rows, there]
            p, o = factor_panel(p, o, lo)
            w_ref[rows, here] = p
            w_ref[rows, there] = o
            if lo + NB < half:
                rest = pl.ds(pl.multiple_of(t * half + lo + NB, NB), half - lo - NB)
                lanes = lax.broadcasted_iota(jnp.int32, (half - lo - NB, half), 1)
                u = p[:, lo + NB:]
                old = jnp.where((lanes >= lo) & (lanes < lo + NB), 0.0, w_ref[rest, here])
                w_ref[rest, here] = old - lax.dot_general(u, p, ROW_CONTRACT, precision=HI, preferred_element_type=jnp.float32)
                w_ref[rest, there] = w_ref[rest, there] - lax.dot_general(u, o, ROW_CONTRACT, precision=HI, preferred_element_type=jnp.float32)

        @pl.when(t == 0)
        def _():
            u = w_ref[:half, half:]
            w_ref[half:, half:] = w_ref[half:, half:] - lax.dot_general(u, u, ROW_CONTRACT, precision=HI, preferred_element_type=jnp.float32)
            done = lower_mask(w_ref[:half, :half])
            w_ref[half:, :half] = -lax.dot_general(u, done, ROW_CONTRACT, precision=HI, preferred_element_type=jnp.float32)


def lower_mask(x):
    r = lax.broadcasted_iota(jnp.int32, x.shape, 0)
    c = lax.broadcasted_iota(jnp.int32, x.shape, 1)
    return jnp.where(r >= c, x, 0.0)


def cholesky_inverse_kernel(g_ref, o_ref, work):
    work[...] = g_ref[...]
    chol_inverse(work)
    o_ref[...] = lower_mask(work[...])


def cholesky_inverse(gram):
    return pl.pallas_call(
        cholesky_inverse_kernel,
        out_shape=jax.ShapeDtypeStruct(gram.shape, jnp.float32),
        in_specs=[pl.BlockSpec(memory_space=pltpu.VMEM)],
        out_specs=pl.BlockSpec(memory_space=pltpu.VMEM),
        scratch_shapes=[pltpu.VMEM(gram.shape, jnp.float32)],
    )(gram)


def apply_inverse(y_loc, factor_inv):
    return lax.dot_general(y_loc, factor_inv, (((1,), (1,)), ((), ())), precision=HI, preferred_element_type=jnp.float32)


def group_sum(part, devices):
    strips = lax.all_to_all(part.reshape(devices, part.shape[0] // devices, part.shape[1]), GRID_AXES, split_axis=0, concat_axis=0)
    return lax.all_gather(jnp.sum(strips, axis=0), GRID_AXES, axis=0, tiled=True)


def orthonormalize(y_loc, total_rows, devices):
    def one_pass(which, y_cur):
        y_low = y_cur.astype(jnp.bfloat16)
        gram_low = lax.dot_general(y_low, y_low, ROW_CONTRACT, preferred_element_type=jnp.float32)
        gram_full = lax.dot_general(y_cur, y_cur, ROW_CONTRACT, precision=HI, preferred_element_type=jnp.float32)
        gram = group_sum(jnp.where(which == 0, gram_low, gram_full), devices) / total_rows
        return apply_inverse(y_cur, cholesky_inverse(gram))

    return lax.fori_loop(0, 2, one_pass, y_loc)


def lower_half(err):
    r = lax.broadcasted_iota(jnp.int32, err.shape, 0)
    c = lax.broadcasted_iota(jnp.int32, err.shape, 1)
    return jnp.where(r > c, err, jnp.where(r == c, 0.5 * err, 0.0))


def eye(size):
    return jnp.where(lax.broadcasted_iota(jnp.int32, (size, size), 0) == lax.broadcasted_iota(jnp.int32, (size, size), 1), 1.0, 0.0)


def mul(a, b):
    return jnp.dot(a, b, precision=HI, preferred_element_type=jnp.float32)


def mul_t(a, b):
    return lax.dot_general(a, b, (((1,), (1,)), ((), ())), precision=HI, preferred_element_type=jnp.float32)


def subspace_kernel(dims, total_rows, shift_ref, a_hbm, start_ref, x_ref, h_ref, flag_ref,
                    a_buf, xlow, xbuf, acc, gloc, slots, red, gsum, work,
                    a_sem, send_near, recv_near, send_far, recv_far, send_line, recv_line, send_end, recv_end,
                    send_core, recv_core, send_rs, recv_rs, send_bc, recv_bc):
    rows_y, cols, rows = dims
    chips_x = cols // 2
    half = rows // 2
    row, col = lax.axis_index("row"), lax.axis_index("col")
    chip, core = lax.div(col, 2), lax.rem(col, 2)
    size = x_ref.shape[1]
    lanes = size // 2
    strip = size // (rows_y * cols)

    def place(dx, dy):
        return lax.rem(chip + dx + chips_x, chips_x), lax.rem(row + dy + rows_y, rows_y)

    def device(dx, dy, flip=False):
        px, py = place(dx, dy)
        return {"row": py, "col": px * 2 + ((1 - core) if flip else core)}

    def slot(dx, dy):
        px, py = place(dx, dy)
        return py * chips_x + px

    def axis_pair(h, u, v):
        return (u, v) if h == 0 else (v, u)

    peers = [(dx, dy, flip) for dx in LINE for dy in LINE for flip in (False, True) if (dx, dy, flip) != (0, 0, False)]
    peers.sort(key=lambda peer: -(2 * abs(peer[0]) + 2 * abs(peer[1]) + peer[2]))
    barrier = pltpu.get_barrier_semaphore()
    for peer in peers:
        pl.semaphore_signal(barrier, inc=1, device_id=device(*peer), device_id_type=MESH_ID)
    pl.semaphore_wait(barrier, len(peers))

    load = pltpu.make_async_copy(a_hbm, a_buf, a_sem)
    load.start()

    def gather_product():
        sent = []

        def send(src, dst, ssem, rsem, dev):
            copy = pltpu.make_async_remote_copy(src_ref=src, dst_ref=dst, send_sem=ssem, recv_sem=rsem, device_id=dev, device_id_type=MESH_ID)
            copy.start()
            sent.append(copy)
            return copy

        base = pl.multiple_of(core * rows, 32)

        def unit(h, dx, dy, lane=None):
            where = pl.ds(pl.multiple_of(slot(dx, dy) * (2 * rows) + base + h * half, 16), half)
            if lane is None:
                return xbuf.at[where, :]
            return xbuf.at[where, pl.ds(lane * lanes, lanes)]

        def own(h):
            return xlow.at[pl.ds(h * half, half), :]

        near, far, line, end, cross = {}, {}, {}, {}, {}
        signs = (1, -1)

        def start_near(h, d):
            near[h, d] = send(own(h), unit(h, 0, 0), send_near.at[h, (d + 1) // 2], recv_near.at[h, (d + 1) // 2], device(*axis_pair(h, d, 0)))

        def start_far(h):
            far[h] = send(own(h), unit(h, 0, 0), send_far.at[h], recv_far.at[h], device(*axis_pair(h, 2, 0)))

        def start_line(h, u):
            piece = unit(h, *axis_pair(h, u, 0))
            source = own(h) if u == 0 else piece
            for d in signs:
                line[h, u, d] = send(source, piece, send_line.at[h, u + 1, (d + 1) // 2], recv_line.at[h, u + 1, (d + 1) // 2],
                                     device(*axis_pair(h, 0, d)))
            if u in STRAIGHT:
                end[h, u, 1] = send(source, piece, send_end.at[h, u + 1, 0], recv_end.at[h, u + 1, 0], device(*axis_pair(h, 0, 2)))

        def start_end(h, u, d):
            piece = unit(h, *axis_pair(h, u, -d), lane=(d + 1) // 2)
            end[h, u, d] = send(piece, piece, send_end.at[h, u + 1, (d + 1) // 2], recv_end.at[h, u + 1, (d + 1) // 2], device(*axis_pair(h, 0, d)))

        def start_cross(h, dx, dy):
            piece = unit(h, dx, dy)
            index = (dy + 1) * 4 + dx + 1
            cross[h, dx, dy] = send(own(h) if (dx, dy) == (0, 0) else piece, piece, send_core.at[h, index], recv_core.at[h, index], device(0, 0, True))

        def product(others, dy, first=False):
            for dx in ((2,) if others else (0, 1, -1)):
                for h in (0, 1):
                    cross[h, dx, dy].wait_recv()
            pair = lax.div(slot(2 if others else 0, dy), 2)
            block = xbuf[pl.ds(pl.multiple_of(pair * (4 * rows), 32), 4 * rows), :]
            term = jnp.dot(a_buf[pair], block, preferred_element_type=jnp.float32)
            acc[...] = term if first else acc[...] + term

        def got_line(us):
            for u in us:
                for d in signs:
                    for h in (0, 1):
                        line[h, u, d].wait_recv()
                        if u not in STRAIGHT:
                            start_end(h, u, d)
                        start_cross(h, *axis_pair(h, u, -d))

        def got_end(us):
            for u in us:
                for h in (0, 1):
                    for d in signs:
                        if (h, u, d) in end:
                            end[h, u, d].wait_recv()
                    start_cross(h, *axis_pair(h, u, 2))

        def got_far():
            for h in (0, 1):
                far[h].wait_recv()
                start_line(h, 2)
                start_cross(h, *axis_pair(h, 2, 0))

        for d in signs:
            for h in (0, 1):
                start_near(h, d)
        for h in (0, 1):
            start_far(h)
        for h in (0, 1):
            start_line(h, 0)
            start_cross(h, 0, 0)
        xbuf[pl.ds(pl.multiple_of(slot(0, 0) * (2 * rows) + base, 32), rows), :] = xlow[...]
        for d in signs:
            for h in (0, 1):
                near[h, d].wait_recv()
                start_line(h, -d)
                start_cross(h, *axis_pair(h, -d, 0))
        got_far()
        got_line((0,))
        got_line((1, -1))
        product(False, 0, first=True)
        got_end((0,))
        got_line((2,))
        product(True, 0)
        for u in signs:
            product(False, u)
        got_end((1, -1))
        got_end((2,))
        for u in signs:
            product(True, u)
        product(False, 2)
        product(True, 2)
        for copy in sent:
            copy.wait_send()

    def strip_of(dx, dy, flip):
        px, py = place(dx, dy)
        return py * cols + px * 2 + ((1 - core) if flip else core)

    def strip_rows(index):
        return pl.ds(pl.multiple_of(index * strip, 8), strip)

    mine = strip_of(0, 0, False)

    def send(src, dst, ssem, rsem, dev):
        copy = pltpu.make_async_remote_copy(src_ref=src, dst_ref=dst, send_sem=ssem, recv_sem=rsem, device_id=dev, device_id_type=MESH_ID)
        copy.start()
        return copy

    class GroupSum:
        def __init__(self, n):
            self.n = n
            self.sent = []
            self.waits = [send(gloc.at[n, strip_rows(strip_of(*peer)), :], slots.at[n, mine], send_rs.at[n, i], recv_rs.at[n, i], device(*peer))
                          for i, peer in enumerate(peers)]
            slots[n, mine] = gloc[n, strip_rows(mine), :]

        def arrive(self):
            for copy in self.waits:
                copy.wait_recv()
            self.sent += self.waits
            self.waits = []

        def spread(self):
            n = self.n
            self.arrive()
            red[n] = jnp.sum(slots[n], axis=0)
            self.waits = [send(red.at[n], gsum.at[n, strip_rows(mine), :], send_bc.at[n, i], recv_bc.at[n, i], device(*peer))
                          for i, peer in enumerate(peers)]
            gsum[n, strip_rows(mine), :] = red[n]

        def finish(self):
            for copy in self.sent:
                copy.wait_send()

    scale = 1.0 / total_rows
    unit_mat = eye(size)

    def sweep(t):
        gather_product()
        y_val = acc[...] - shift_ref[t] * x_ref[...]
        y_low = y_val.astype(jnp.bfloat16)
        gloc[0] = lax.dot_general(y_low, y_low, ROW_CONTRACT, preferred_element_type=jnp.float32)
        one = GroupSum(0)
        acc[...] = y_val
        gloc[1] = lax.dot_general(y_val, y_val, ROW_CONTRACT, precision=HI, preferred_element_type=jnp.float32)
        two = GroupSum(1)
        one.spread()
        two.spread()
        one.arrive()
        work[...] = gsum[0] * scale
        chol_inverse(work)
        two.arrive()
        first = lower_mask(work[...])
        gram_two = mul_t(mul(first, gsum[1] * scale), first)
        err = gram_two - unit_mat
        far_one = jnp.where(jnp.sum(err * err, axis=(0, 1), keepdims=True) <= FIRST_ERR, 0.0, 1.0)
        second = unit_mat - lower_half(err)
        near_x = mul_t(acc[...], mul(second, first))
        err = mul_t(mul(second, gram_two), second) - unit_mat
        far_two = jnp.where(jnp.sum(err * err, axis=(0, 1), keepdims=True) <= SECOND_ERR, 0.0, 1.0)
        flag_ref[...] = jnp.maximum(flag_ref[...], jnp.maximum(far_one, far_two))
        x_val = near_x - mul_t(near_x, lower_half(err))
        xlow[...] = x_val.astype(jnp.bfloat16)
        x_ref[...] = x_val
        one.finish()
        two.finish()

    flag_ref[...] = jnp.zeros_like(flag_ref)
    x_ref[...] = start_ref[...]
    xlow[...] = start_ref[...].astype(jnp.bfloat16)
    load.wait()

    @pl.loop(0, shift_ref.shape[0])
    def _(t):
        sweep(t)

    gather_product()
    gloc[0] = lax.dot_general(x_ref[...], acc[...], ROW_CONTRACT, precision=HI, preferred_element_type=jnp.float32)
    total = GroupSum(0)
    total.spread()
    total.arrive()
    h_ref[...] = gsum[0] / total_rows
    total.finish()


def iterate(dims, total_rows, shifts, a_blocks, x_start):
    rows_y, cols, rows = dims
    size = x_start.shape[1]
    chips = rows_y * cols // 2
    dma = pltpu.SemaphoreType.DMA
    vmem = pl.BlockSpec(memory_space=pltpu.VMEM)
    peers = 2 * chips - 1
    strip = size // (2 * chips)
    return pl.pallas_call(
        functools.partial(subspace_kernel, dims, total_rows),
        out_shape=(
            jax.ShapeDtypeStruct((rows, size), jnp.float32),
            jax.ShapeDtypeStruct((size, size), jnp.float32),
            jax.ShapeDtypeStruct((8, 128), jnp.float32),
        ),
        in_specs=[pl.BlockSpec(memory_space=pltpu.SMEM), pl.BlockSpec(memory_space=pl.ANY), vmem],
        out_specs=(vmem,) * 3,
        scratch_shapes=[
            pltpu.VMEM(a_blocks.shape, jnp.bfloat16),
            pltpu.VMEM((rows, size), jnp.bfloat16),
            pltpu.VMEM((chips * 2 * rows, size), jnp.bfloat16),
            pltpu.VMEM((rows, size), jnp.float32),
            pltpu.VMEM((2, size, size), jnp.float32),
            pltpu.VMEM((2, 2 * chips, strip, size), jnp.float32),
            pltpu.VMEM((2, strip, size), jnp.float32),
            pltpu.VMEM((2, size, size), jnp.float32),
            pltpu.VMEM((size, size), jnp.float32),
            dma,
            dma((2, 2)), dma((2, 2)), dma((2,)), dma((2,)),
            dma((2, 4, 2)), dma((2, 4, 2)), dma((2, 4, 2)), dma((2, 4, 2)),
            dma((2, 16)), dma((2, 16)),
            dma((2, peers)), dma((2, peers)), dma((2, peers)), dma((2, peers)),
        ],
        compiler_params=pltpu.CompilerParams(collective_id=0, has_side_effects=True, vmem_limit_bytes=56 * 2**20),
        name="subspace_sweeps",
    )(shifts, a_blocks, x_start)


def solution(mesh):
    row_count = mesh.shape["row"]
    col_count = mesh.shape["col"]

    def apply_operator(a_rows, x_loc):
        rows, size = x_loc.shape
        x_parts = x_loc.astype(jnp.bfloat16).reshape(rows, 4, size // 4).transpose(1, 0, 2)
        gathered = lax.map(lambda part: lax.all_gather(part, GRID_AXES, axis=0, tiled=True), x_parts)
        x_full = gathered.transpose(1, 0, 2).reshape(gathered.shape[1], size)
        return jnp.dot(a_rows, x_full, preferred_element_type=jnp.float32)

    def careful_program(a_blocks, x_loc, shift_vec, total_rows):
        a_rows = a_blocks.transpose(1, 0, 2).reshape(x_loc.shape[0], total_rows)

        sweeps = shift_vec.shape[0]

        def sweep(sweep_idx, carry):
            x_cur, _ = carry
            applied = apply_operator(a_rows, x_cur)
            shift = shift_vec[jnp.minimum(sweep_idx, sweeps - 1)]
            x_next = orthonormalize(applied - shift * x_cur, total_rows, row_count * col_count)
            return jnp.where(sweep_idx < sweeps, x_next, x_cur), applied

        x_loc, applied = lax.fori_loop(0, sweeps + 1, sweep, (x_loc, x_loc))
        local_part = lax.dot_general(x_loc, applied, ROW_CONTRACT, precision=HI, preferred_element_type=jnp.float32)
        return x_loc, group_sum(local_part, row_count * col_count) / total_rows

    def local_program(a_blk, x_start, shift_vec):
        total_rows = a_blk.shape[0] * row_count
        rows = x_start.shape[0]
        dims = (row_count, col_count, rows)
        a_blocks = lax.all_to_all(a_blk.reshape(col_count, rows, a_blk.shape[1]), "col", split_axis=0, concat_axis=0)

        x_loc, rayleigh, flag = iterate(dims, total_rows, shift_vec, a_blocks, x_start)
        return lax.cond(
            flag[0, 0] > 0.0,
            lambda: careful_program(a_blocks, x_start, shift_vec, total_rows),
            lambda: (x_loc, rayleigh),
        )

    return jax.shard_map(
        local_program,
        mesh=mesh,
        in_specs=(P(("batch", "row"), "col"), P(("batch", "row", "col"), None), P("batch")),
        out_specs=(P(("batch", "row", "col"), None), P("batch", None)),
        check_vma=False,
    )
```
